32 devices in a mesh: rep: 1 (over z), ep: 4 (over y), fsdp: 8 (over x, core).
Axes of the slice: x: 4, y: 4, z: 1, core: 2. Of those that a mesh axis runs over, the one named last changes fastest.
The devices are a block of a 4x4x8 slice.
Arguments:
- x_in: bfloat16 [16384, 2048], P(('rep', 'ep', 'fsdp'))
- norm_w: float32 [2, 2048], replicated
- router_w: bfloat16 [2, 2048, 4], replicated
- gate_w: bfloat16 [2, 4, 2048, 5632], P(None, 'ep', None, 'fsdp')
- up_w: bfloat16 [2, 4, 2048, 5632], P(None, 'ep', None, 'fsdp')
- down_w: bfloat16 [2, 4, 5632, 2048], P(None, 'ep', 'fsdp')
- routes: int32 [2, 16384, 2], P(None, ('rep', 'ep', 'fsdp'))
Outputs:
- output: bfloat16 [16384, 2048], P(('rep', 'ep', 'fsdp'))
All inputs are finite; a program needn't handle non-finite values.
Results may differ from the reference program's by a relative error of at most 0.012462.
Values are sent between devices in bfloat16 or wider.
A program may use at most 768 MiB of HBM per device.

```python
import jax
import jax.numpy as jnp
from jax import lax
import numpy as np

EXPERTS = 4
TOP = 2
D_MODEL = 2048
FF_DIM = 5632
TOK_DEV = 512
DEV_PART = 32
LAYERS = 2

NORM_EPS = 1e-5
CAPACITY = 8 * ((2 * TOK_DEV * TOP + 8 * EXPERTS - 1) // (8 * EXPERTS))
TOKENS = TOK_DEV * DEV_PART
ROW_CAP = DEV_PART * CAPACITY


def count_pattern(n_pairs, n_experts, capacity):
    counts = [1 + ((capacity - 1) * (n_experts - 1 - position)) // (n_experts - 1) for position in range(n_experts)]
    cursor = 1
    while sum(counts) < n_pairs:
        if counts[cursor] < capacity:
            counts[cursor] += 1
        cursor = cursor % (n_experts - 1) + 1
    while sum(counts) > n_pairs:
        if counts[cursor] > 1:
            counts[cursor] -= 1
        cursor = cursor % (n_experts - 1) + 1
    return counts


def draw_routes(route_key):
    counts = count_pattern(TOK_DEV * TOP, EXPERTS, CAPACITY)
    pattern = np.repeat(np.arange(EXPERTS), counts).astype(np.int32)

    def one_block(block_key):
        key_label, key_order = jax.random.split(block_key)
        relabel = jax.random.permutation(key_label, EXPERTS)
        expert_ids = relabel[pattern].reshape(TOP, TOK_DEV).T
        token_order = jax.random.permutation(key_order, TOK_DEV)
        return expert_ids[token_order]

    block_keys = jax.random.split(route_key, LAYERS * DEV_PART)
    all_blocks = jax.vmap(one_block)(block_keys)
    return all_blocks.reshape(LAYERS, TOKENS, TOP).astype(jnp.int32)


def setup_inputs(seed: int = 0, part: int = 0) -> dict:
    weight_keys = jax.random.split(jax.random.key(seed), 5)
    part_keys = jax.random.split(jax.random.fold_in(jax.random.key(seed + 1), part), 2)
    x_in = jax.random.normal(part_keys[0], (TOKENS, D_MODEL), jnp.float32).astype(jnp.bfloat16)
    norm_w = 1.0 + 0.25 * jax.random.normal(weight_keys[0], (LAYERS, D_MODEL), jnp.float32)
    router_w = (jax.random.normal(weight_keys[1], (LAYERS, D_MODEL, EXPERTS), jnp.float32) * D_MODEL ** -0.5).astype(jnp.bfloat16)
    gate_w = (jax.random.normal(weight_keys[2], (LAYERS, EXPERTS, D_MODEL, FF_DIM), jnp.float32) * D_MODEL ** -0.5).astype(jnp.bfloat16)
    up_w = (jax.random.normal(weight_keys[3], (LAYERS, EXPERTS, D_MODEL, FF_DIM), jnp.float32) * D_MODEL ** -0.5).astype(jnp.bfloat16)
    down_w = (jax.random.normal(weight_keys[4], (LAYERS, EXPERTS, FF_DIM, D_MODEL), jnp.float32) * (1.5 * (TOP / FF_DIM) ** 0.5)).astype(jnp.bfloat16)
    routes = draw_routes(part_keys[1])
    return {"x_in": x_in, "norm_w": norm_w, "router_w": router_w, "gate_w": gate_w, "up_w": up_w, "down_w": down_w, "routes": routes}


def rms_norm(stream, norm_row):
    widened = stream.astype(jnp.float32)
    inv_rms = lax.rsqrt(jnp.mean(widened * widened, axis=-1, keepdims=True) + NORM_EPS)
    return (widened * inv_rms * norm_row).astype(jnp.bfloat16)


def moe_layer(stream, layer_params):
    norm_row, router_l, gate_l, up_l, down_l, routes_l = layer_params
    hidden = rms_norm(stream, norm_row)
    logits = jnp.dot(hidden, router_l, preferred_element_type=jnp.float32)
    gate_probs = jax.nn.softmax(jnp.take_along_axis(logits, routes_l, axis=1), axis=-1)

    def expert_step(mixed_sum, expert_params):
        expert_id, gate_e, up_e, down_e = expert_params
        is_chosen = routes_l == expert_id
        token_gate = jnp.sum(jnp.where(is_chosen, gate_probs, 0.0), axis=1)
        token_rows = jnp.nonzero(jnp.any(is_chosen, axis=1), size=ROW_CAP, fill_value=0)[0]
        row_valid = jnp.arange(ROW_CAP) < jnp.sum(is_chosen)
        row_gate = jnp.where(row_valid, token_gate[token_rows], 0.0)
        picked = hidden[token_rows]
        pre_gate = jnp.dot(picked, gate_e, preferred_element_type=jnp.float32)
        pre_up = jnp.dot(picked, up_e, preferred_element_type=jnp.float32)
        inner_act = (jax.nn.silu(pre_gate) * pre_up).astype(jnp.bfloat16)
        expert_out = jnp.dot(inner_act, down_e, preferred_element_type=jnp.float32).astype(jnp.bfloat16)
        mixed_sum = mixed_sum.at[token_rows].add(row_gate[:, None] * expert_out.astype(jnp.float32))
        return mixed_sum, None

    start_sum = jnp.zeros(stream.shape, jnp.float32)
    mixed_sum, _ = lax.scan(expert_step, start_sum, (jnp.arange(EXPERTS), gate_l, up_l, down_l))
    return (stream.astype(jnp.float32) + mixed_sum).astype(jnp.bfloat16), None


def reference(x_in, norm_w, router_w, gate_w, up_w, down_w, routes):
    final_stream, _ = lax.scan(moe_layer, x_in, (norm_w, router_w, gate_w, up_w, down_w, routes))
    return final_stream
```

```python
import functools

import jax
import jax.numpy as jnp
from jax import lax
from jax.experimental import pallas as pl
from jax.experimental.pallas import tpu as pltpu
from jax.sharding import PartitionSpec as P

MESH = pl.DeviceIdType.MESH
NORM_EPS = 1e-5
CHUNK = 128


def kernel(n_ep, n_fs, x_hbm, norm_ref, router_ref, w1, w3, w2, routes_ref,
           out_hbm, g1, g3, g2, h_land, o_land, r_land,
           h_all, acc, b1, b3, b2, act, xs, orecv, gates,
           ws, wr, hs, hr, os_, or_, ld):
    layers, tok_dev = routes_ref.shape[0], routes_ref.shape[1]
    d_model = x_hbm.shape[1]
    chips = n_fs // 2
    y = lax.axis_index("ep")
    f = lax.axis_index("fsdp")
    xc = f // 2
    core = lax.rem(f, 2)

    def fs_index(dx, dk):
        return lax.rem(xc + dx, chips) * 2 + lax.rem(core + dk, 2)

    right, left, opp, partner = fs_index(1, 0), fs_index(chips - 1, 0), fs_index(2, 0), fs_index(0, 1)
    up, down = lax.rem(y + 1, n_ep), lax.rem(y + n_ep - 1, n_ep)
    to_right, to_left, to_partner = {"fsdp": right}, {"fsdp": left}, {"fsdp": partner}
    to_up, to_down = {"ep": up}, {"ep": down}

    own_refs, land_refs, bufs = (w1, w3, w2), (g1, g3, g2), (b1, b3, b2)

    class Lazy:
        def __init__(self, *args):
            self.args = args

        def start(self):
            remote(*self.args).start()

        def wait_send(self):
            remote(*self.args).wait_send()

    def remote(src, dst, send, recv, dev):
        return pltpu.make_async_remote_copy(src_ref=src, dst_ref=dst, send_sem=send, recv_sem=recv,
                                            device_id=dev, device_id_type=MESH)

    def own(l, t):
        return own_refs[t].at[l, 0]

    def land(l, t, slot):
        return land_refs[t].at[l, slot]

    def half(ref, i):
        rows = ref.shape[0] // 2
        return ref.at[pl.ds(i * rows, rows)]

    def weight_copies(l, t):
        return (
            Lazy(own(l, t), land(l, t, f), ws.at[l, t, 0], wr.at[l, t, 2], to_right),
            Lazy(own(l, t), land(l, t, f), ws.at[l, t, 1], wr.at[l, t, 3], to_left),
            Lazy(own(l, t), land(l, t, f), ws.at[l, t, 2], wr.at[l, t, 1], to_partner),
            Lazy(half(land(l, t, left), 0), half(land(l, t, left), 0), ws.at[l, t, 3], wr.at[l, t, 6], to_right),
            Lazy(half(land(l, t, right), 1), half(land(l, t, right), 1), ws.at[l, t, 4], wr.at[l, t, 8], to_left),
            Lazy(land(l, t, left), land(l, t, left), ws.at[l, t, 5], wr.at[l, t, 4], to_partner),
            Lazy(land(l, t, right), land(l, t, right), ws.at[l, t, 6], wr.at[l, t, 5], to_partner),
            Lazy(half(land(l, t, opp), 0), half(land(l, t, opp), 0), ws.at[l, t, 7], wr.at[l, t, 7], to_partner),
            Lazy(half(land(l, t, opp), 1), half(land(l, t, opp), 1), ws.at[l, t, 8], wr.at[l, t, 9], to_partner),
        )

    def wait_weight(l, t, slot, sem):
        ref = land(l, t, slot)
        remote(ref, ref, ws.at[l, t, 0], wr.at[l, t, sem], to_partner).wait_recv()

    def wait_weight_half(l, t, slot, i, sem):
        ref = half(land(l, t, slot), i)
        remote(ref, ref, ws.at[l, t, 0], wr.at[l, t, sem], to_partner).wait_recv()

    def push_own(l, t):
        for copy in weight_copies(l, t)[:3]:
            copy.start()

    def pass_sides(l, t):
        wait_weight(l, t, left, 2)
        wait_weight(l, t, right, 3)
        for copy in weight_copies(l, t)[3:7]:
            copy.start()

    def pass_opp(l, t):
        wait_weight_half(l, t, opp, 0, 6)
        wait_weight_half(l, t, opp, 1, 8)
        for copy in weight_copies(l, t)[7:9]:
            copy.start()

    def slot_of(s):
        c = s // 2
        dx = jnp.minimum(c, 1) * (lax.rem(c + 1, 3) + 1)
        return fs_index(dx, lax.rem(s, 2))

    def load(l, t, s):
        @pl.when(s == 1)
        def _():
            wait_weight(l, t, partner, 1)

        @pl.when(s == 3)
        def _():
            wait_weight(l, t, fs_index(chips - 1, 1), 4)

        @pl.when(s == 5)
        def _():
            wait_weight(l, t, fs_index(1, 1), 5)

        @pl.when(s == 6)
        def _():
            pass_opp(l, t)

        @pl.when(s == 7)
        def _():
            wait_weight_half(l, t, fs_index(2, 1), 0, 7)
            wait_weight_half(l, t, fs_index(2, 1), 1, 9)

        @pl.when(s == 0)
        def _():
            pltpu.make_async_copy(own(l, t), bufs[t], ld.at[t]).start()

        @pl.when(s > 0)
        def _():
            pltpu.make_async_copy(land(l, t, slot_of(s)), bufs[t], ld.at[t]).start()

    def load_wait(t):
        pltpu.make_async_copy(own(0, t), bufs[t], ld.at[t]).wait()

    barrier = pltpu.get_barrier_semaphore()
    for dev in (to_right, to_left, to_partner, to_up, to_down):
        pl.semaphore_signal(barrier, inc=1, device_id=dev, device_id_type=MESH)
    pl.semaphore_wait(barrier, 5)

    x_copy = pltpu.make_async_copy(x_hbm, xs, ld.at[3])
    x_copy.start()
    for t in range(3):
        push_own(0, t)
    x_copy.wait()

    def normalise(l):
        def step(i, carry):
            rows = pl.ds(pl.multiple_of(i * CHUNK, CHUNK), CHUNK)
            wide = xs[rows, :].astype(jnp.float32)
            inv = lax.rsqrt(jnp.mean(wide * wide, axis=-1, keepdims=True) + NORM_EPS)
            hidden = (wide * inv * norm_ref[l]).astype(jnp.bfloat16)
            h_all[0, rows, :] = hidden
            logits = jnp.dot(hidden, router_ref[l], preferred_element_type=jnp.float32)
            lane = lax.broadcasted_iota(jnp.int32, logits.shape, 1)
            ids = routes_ref[l, rows, :]
            pick0 = jnp.sum(jnp.where(lane == ids[:, 0:1], logits, 0.0), axis=-1, keepdims=True)
            pick1 = jnp.sum(jnp.where(lane == ids[:, 1:2], logits, 0.0), axis=-1, keepdims=True)
            top = jnp.maximum(pick0, pick1)
            e0, e1 = jnp.exp(pick0 - top), jnp.exp(pick1 - top)
            total = e0 + e1
            gates[rows, :] = jnp.where(lane == 0, e0 / total, e1 / total)
            return carry
        lax.fori_loop(0, tok_dev // CHUNK, step, 0)

    def hidden_copies(l):
        return (
            Lazy(h_all.at[0], h_land.at[l, 0], hs.at[l, 0], hr.at[l, 0], to_up),
            Lazy(h_all.at[0], h_land.at[l, 1], hs.at[l, 1], hr.at[l, 1], to_down),
            Lazy(half(h_land.at[l, 0], 0), half(h_land.at[l, 2], 0), hs.at[l, 2], hr.at[l, 2], to_up),
            Lazy(half(h_land.at[l, 1], 1), half(h_land.at[l, 2], 1), hs.at[l, 3], hr.at[l, 3], to_down),
        )

    def send_hidden(l):
        for copy in hidden_copies(l)[:2]:
            copy.start()

    def take_hidden(l, between):
        copies = hidden_copies(l)
        for i in (0, 1):
            remote(h_land.at[l, i], h_land.at[l, i], hs.at[l, i], hr.at[l, i], to_up).wait_recv()
            copies[2 + i].start()
            pltpu.make_async_copy(h_land.at[l, i], h_all.at[1 + i], ld.at[4 + i]).start()
        between()
        for i in (0, 1):
            ref = half(h_land.at[l, 2], i)
            remote(ref, ref, hs.at[l, 2 + i], hr.at[l, 2 + i], to_up).wait_recv()
        pltpu.make_async_copy(h_land.at[l, 2], h_all.at[3], ld.at[6]).start()
        for i in range(3):
            pltpu.make_async_copy(h_land.at[l, i], h_all.at[1 + i], ld.at[4 + i]).wait()
        for copy in copies:
            copy.wait_send()

    def clear_acc():
        def step(i, carry):
            rows = pl.ds(pl.multiple_of(lax.rem(i, 4) * CHUNK, CHUNK), CHUNK)
            acc[i // 4, rows, :] = jnp.zeros((CHUNK, d_model), jnp.float32)
            return carry
        lax.fori_loop(0, 4 * (tok_dev // CHUNK), step, 0)

    def experts(l):
        def slice_step(s, carry):
            load_wait(0)
            load_wait(1)

            def gate_up(rb, c):
                @pl.when(rb == 2)
                def _():
                    if l == 0:
                        @pl.when(s == 2)
                        def _():
                            pass_sides(l, 2)
                    load(l, 2, s)
                    if l == 0:
                        @pl.when(s == 4)
                        def _():
                            for t in range(3):
                                push_own(1, t)
                u = jnp.dot(h_all[rb], b1[...], preferred_element_type=jnp.float32)
                v = jnp.dot(h_all[rb], b3[...], preferred_element_type=jnp.float32)
                act[rb] = (u * jax.nn.sigmoid(u) * v).astype(jnp.bfloat16)
                return c
            lax.fori_loop(0, 4, gate_up, 0)

            if l == 0:
                @pl.when(s == 1)
                def _():
                    pass_sides(l, 0)
                    pass_sides(l, 1)

            @pl.when(s < 7)
            def _():
                load(l, 0, s + 1)
                load(l, 1, s + 1)
            load_wait(2)

            def down_proj(rb, c):
                cols = 512
                for n in range(d_model // cols):
                    part = pl.ds(n * cols, cols)
                    acc[rb, :, part] += jnp.dot(act[rb], b2[:, part], preferred_element_type=jnp.float32)
                return c
            lax.fori_loop(0, 4, down_proj, 0)
            return carry

        load(l, 0, 0)
        load(l, 1, 0)
        lax.fori_loop(0, 8, slice_step, 0)

    def round_block(block):
        def step(i, carry):
            rows = pl.ds(pl.multiple_of(i * CHUNK, CHUNK), CHUNK)
            h_all[block, rows, :] = acc[block, rows, :].astype(jnp.bfloat16)
            return carry
        lax.fori_loop(0, tok_dev // CHUNK, step, 0)

    def output_copies(l):
        return (
            Lazy(half(h_all.at[3], 0), r_land.at[l, 0], os_.at[l, 0], or_.at[l, 0], to_up),
            Lazy(half(h_all.at[3], 1), r_land.at[l, 1], os_.at[l, 1], or_.at[l, 1], to_down),
            Lazy(h_all.at[1], o_land.at[l, 0], os_.at[l, 2], or_.at[l, 2], to_down),
            Lazy(h_all.at[2], o_land.at[l, 1], os_.at[l, 3], or_.at[l, 3], to_up),
            Lazy(r_land.at[l, 0], half(o_land.at[l, 2], 0), os_.at[l, 4], or_.at[l, 4], to_up),
            Lazy(r_land.at[l, 1], half(o_land.at[l, 2], 1), os_.at[l, 5], or_.at[l, 5], to_down),
        )

    def return_outputs(l):
        copies = output_copies(l)
        round_block(3)
        copies[0].start()
        copies[1].start()
        round_block(1)
        copies[2].start()
        round_block(2)
        copies[3].start()
        for i in (0, 1):
            ref = r_land.at[l, i]
            remote(ref, ref, os_.at[l, i], or_.at[l, i], to_up).wait_recv()
            copies[4 + i].start()
        for i in (0, 1):
            ref = o_land.at[l, i]
            remote(ref, ref, os_.at[l, i], or_.at[l, 2 + i], to_up).wait_recv()
            pltpu.make_async_copy(ref, orecv.at[i], ld.at[4 + i]).start()
        for i in (0, 1):
            ref = half(o_land.at[l, 2], i)
            remote(ref, ref, os_.at[l, i], or_.at[l, 4 + i], to_up).wait_recv()
        pltpu.make_async_copy(o_land.at[l, 2], orecv.at[2], ld.at[6]).start()
        for i in range(3):
            pltpu.make_async_copy(o_land.at[l, i], orecv.at[i], ld.at[4 + i]).wait()
        for copy in copies:
            copy.wait_send()

    def combine(l):
        sources = (up, down, lax.rem(y + 2, n_ep))

        def step(i, carry):
            rows = pl.ds(pl.multiple_of(i * CHUNK, CHUNK), CHUNK)
            ids, gate = routes_ref[l, rows, :], gates[rows, :]
            id0, id1, gate0, gate1 = ids[:, 0:1], ids[:, 1:2], gate[:, 0:1], gate[:, 1:2]

            def term(expert, value):
                is0, is1 = id0 == expert, id1 == expert
                weight = jnp.where(is0, gate0, gate1)
                return jnp.where(jnp.logical_or(is0, is1), weight * value.astype(jnp.float32), 0.0)
            mixed = term(y, acc[0, rows, :].astype(jnp.bfloat16))
            for j, expert in enumerate(sources):
                mixed += term(expert, orecv[j, rows, :])
            xs[rows, :] = (xs[rows, :].astype(jnp.float32) + mixed).astype(jnp.bfloat16)
            return carry
        lax.fori_loop(0, tok_dev // CHUNK, step, 0)

    normalise(0)
    send_hidden(0)
    clear_acc()
    take_hidden(0, lambda: None)
    experts(0)
    return_outputs(0)
    combine(0)
    normalise(1)
    send_hidden(1)
    clear_acc()
    pass_sides(1, 0)
    take_hidden(1, lambda: pass_sides(1, 1))
    pass_sides(1, 2)
    experts(1)
    return_outputs(1)
    combine(1)
    out_copy = pltpu.make_async_copy(xs, out_hbm, ld.at[3])
    out_copy.start()
    for l in range(layers):
        for t in range(3):
            for copy in weight_copies(l, t):
                copy.wait_send()
    out_copy.wait()


def solution(mesh):
    n_ep, n_fs = mesh.shape["ep"], mesh.shape["fsdp"]
    token_spec = P(("rep", "ep", "fsdp"), None)
    expert_in_spec = P(None, "ep", None, "fsdp")
    expert_out_spec = P(None, "ep", "fsdp", None)
    route_spec = P(None, ("rep", "ep", "fsdp"), None)

    def device_step(x_in, norm_w, router_w, gate_w, up_w, down_w, routes):
        layers, tok_dev, top_k = routes.shape
        d_model = x_in.shape[1]
        ff = gate_w.shape[3]
        router_pad = jnp.pad(router_w, ((0, 0), (0, 0), (0, 128 - router_w.shape[2])))
        bf16 = jnp.bfloat16
        hbm, vmem = pl.BlockSpec(memory_space=pl.ANY), pl.BlockSpec(memory_space=pltpu.VMEM)
        shape = jax.ShapeDtypeStruct
        outs = pl.pallas_call(
            functools.partial(kernel, n_ep, n_fs),
            name="moe_layers",
            out_shape=(shape((tok_dev, d_model), bf16),
                       shape((layers, n_fs, d_model, ff), bf16),
                       shape((layers, n_fs, d_model, ff), bf16),
                       shape((layers, n_fs, ff, d_model), bf16),
                       shape((layers, 3, tok_dev, d_model), bf16),
                       shape((layers, 3, tok_dev, d_model), bf16),
                       shape((layers, 2, tok_dev // 2, d_model), bf16)),
            in_specs=[hbm, vmem, vmem, hbm, hbm, hbm, vmem],
            out_specs=(hbm,) * 7,
            scratch_shapes=[
                pltpu.VMEM((4, tok_dev, d_model), bf16),
                pltpu.VMEM((4, tok_dev, d_model), jnp.float32),
                pltpu.VMEM((d_model, ff), bf16),
                pltpu.VMEM((d_model, ff), bf16),
                pltpu.VMEM((ff, d_model), bf16),
                pltpu.VMEM((4, tok_dev, ff), bf16),
                pltpu.VMEM((tok_dev, d_model), bf16),
                pltpu.VMEM((3, tok_dev, d_model), bf16),
                pltpu.VMEM((tok_dev, 128), jnp.float32),
                pltpu.SemaphoreType.DMA((layers, 3, 9)),
                pltpu.SemaphoreType.DMA((layers, 3, 10)),
                pltpu.SemaphoreType.DMA((layers, 4)),
                pltpu.SemaphoreType.DMA((layers, 4)),
                pltpu.SemaphoreType.DMA((layers, 6)),
                pltpu.SemaphoreType.DMA((layers, 6)),
                pltpu.SemaphoreType.DMA((7,)),
            ],
            compiler_params=pltpu.CompilerParams(collective_id=0, has_side_effects=True,
                                                 vmem_limit_bytes=66_000_000),
        )(x_in, norm_w[:, None, :], router_pad, gate_w, up_w, down_w, routes)
        return outs[0]

    return jax.shard_map(device_step, mesh=mesh,
                         in_specs=(token_spec, P(), P(), expert_in_spec, expert_in_spec, expert_out_spec, route_spec),
                         out_specs=token_spec, check_vma=False)
```

```python
import functools

import jax
import jax.numpy as jnp
from jax import lax
from jax.experimental import pallas as pl
from jax.experimental.pallas import tpu as pltpu
from jax.sharding import PartitionSpec as P

MESH = pl.DeviceIdType.MESH
NORM_EPS = 1e-5
NT = (((1,), (1,)), ((), ()))
CHUNK = 128


def kernel(n_ep, n_fs, x_hbm, norm_ref, router_ref, w1, w3, w2, routes_ref,
           out_hbm, g1, g3, g2, h_land, o_land, r_land,
           h_all, acc, b13, b2, act, xs, orecv, gates,
           ws, wr, hs, hr, os_, or_, ld):
    layers, tok_dev = routes_ref.shape[0], routes_ref.shape[1]
    d_model, ff = x_hbm.shape[1], w2.shape[2]
    part = tok_dev // 2
    chips = n_fs // 2
    y = lax.axis_index("ep")
    f = lax.axis_index("fsdp")
    xc = f // 2
    core = lax.rem(f, 2)

    def ring_slot(r, k):
        return lax.rem(xc + (1 - k) * (chips - r) + k * r, chips) * 2 + k

    def slot_of(s):
        return ring_slot(s // 2, lax.rem(core + lax.rem(s, 2), 2))

    following, previous, partner = ring_slot(chips - 1, core), ring_slot(1, core), xc * 2 + 1 - core
    up, down = lax.rem(y + 1, n_ep), lax.rem(y + n_ep - 1, n_ep)
    to_next, to_prev, to_partner = {"fsdp": following}, {"fsdp": previous}, {"fsdp": partner}
    to_up, to_down = {"ep": up}, {"ep": down}

    def remote(src, dst, send, recv, dev):
        return pltpu.make_async_remote_copy(src_ref=src, dst_ref=dst, send_sem=send, recv_sem=recv,
                                            device_id=dev, device_id_type=MESH)

    own_refs, land_refs = (w1, w3, w2), (g1, g3, g2)

    def land(l, t, slot):
        return land_refs[t].at[l, slot]

    def source(l, t, r):
        return own_refs[t].at[l, 0] if r == 0 else land(l, t, slot_of(2 * r))

    def ring_send(l, t, r):
        return remote(source(l, t, r), land(l, t, slot_of(2 * r)), ws.at[l, t, r], wr.at[l, t, 2 * r + 2], to_next)

    def partner_send(l, t, r):
        return remote(source(l, t, r), land(l, t, slot_of(2 * r)), ws.at[l, t, 3 + r], wr.at[l, t, 2 * r + 1],
                      to_partner)

    def arrived(l, t, s):
        ref = land(l, t, slot_of(s))
        remote(ref, ref, ws.at[l, t, 0], wr.at[l, t, s], to_partner).wait_recv()

    def push_own(l, t):
        ring_send(l, t, 0).start()
        partner_send(l, t, 0).start()

    def pass_ring(l, t, r):
        arrived(l, t, 2 * r)
        if r < 3:
            ring_send(l, t, r).start()
        partner_send(l, t, r).start()

    main = ff // 128 * 128
    tail = ff - main
    groups = [(c, min(256, main - c)) for c in range(0, main, 256)] + [(main, tail)]

    def load13(l, s, i):
        def start(refs):
            for c, width in groups:
                for k in (0, 1):
                    pltpu.make_async_copy(refs[k].at[pl.ds(c, width)],
                                          b13.at[lax.rem(i, 2), pl.ds(2 * c + k * width, width)], ld.at[0]).start()

        @pl.when(s == 0)
        def _():
            start((w1.at[l, 0], w3.at[l, 0]))

        @pl.when(s > 0)
        def _():
            start((land(l, 0, slot_of(s)), land(l, 1, slot_of(s))))

    def load13_wait():
        pltpu.make_async_copy(b13.at[0], b13.at[0], ld.at[0]).wait()

    def load2(l, s):
        @pl.when(s == 0)
        def _():
            pltpu.make_async_copy(w2.at[l, 0], b2, ld.at[1]).start()

        @pl.when(s > 0)
        def _():
            pltpu.make_async_copy(g2.at[l, slot_of(s)], b2, ld.at[1]).start()

    def load2_wait():
        pltpu.make_async_copy(g2.at[0, 0], b2, ld.at[1]).wait()

    def place(block, q):
        return h_all.at[2 * q + block // 2, pl.ds(block % 2 * part, part)]

    def normalise(l, q):
        def step(i, carry):
            rows = pl.ds(pl.multiple_of(q * part + i * CHUNK, CHUNK), CHUNK)
            wide = xs[rows, :].astype(jnp.float32)
            inv = lax.rsqrt(jnp.mean(wide * wide, axis=-1, keepdims=True) + NORM_EPS)
            hidden = (wide * inv * norm_ref[l:l + 1, :]).astype(jnp.bfloat16)
            h_all[2 * q, pl.ds(pl.multiple_of(i * CHUNK, CHUNK), CHUNK), :] = hidden
            logits = lax.dot_general(hidden, router_ref[l], NT, preferred_element_type=jnp.float32)
            lane = lax.broadcasted_iota(jnp.int32, logits.shape, 1)
            ids = routes_ref[l, rows, :]
            pick0 = jnp.sum(jnp.where(lane == ids[:, 0:1], logits, 0.0), axis=-1, keepdims=True)
            pick1 = jnp.sum(jnp.where(lane == ids[:, 1:2], logits, 0.0), axis=-1, keepdims=True)
            top = jnp.maximum(pick0, pick1)
            e0, e1 = jnp.exp(pick0 - top), jnp.exp(pick1 - top)
            total = e0 + e1
            gates[rows, :] = jnp.where(lax.broadcasted_iota(jnp.int32, (CHUNK, 128), 1) == 0, e0 / total, e1 / total)
            return carry
        lax.fori_loop(0, part // CHUNK, step, 0)

    def half(ref, i):
        rows = ref.shape[0] // 2
        return ref.at[pl.ds(i * rows, rows)]

    def send_side(l, q, i):
        return remote(place(0, q), h_land.at[l, q, i], hs.at[l, q, i], hr.at[l, q, i], (to_up, to_down)[i])

    def send_far(l, q, i):
        return remote(half(h_land.at[l, q, i], i), half(h_land.at[l, q, 2], i), hs.at[l, q, 2 + i],
                      hr.at[l, q, 2 + i], (to_up, to_down)[i])

    def send_hidden(l, q):
        for i in (0, 1):
            send_side(l, q, i).start()

    def hidden_load(l, q, i):
        return pltpu.make_async_copy(h_land.at[l, q, i], place(1 + i, q), ld.at[4 + i])

    def take_sides(l, q):
        for i in (0, 1):
            ref = h_land.at[l, q, i]
            remote(ref, ref, hs.at[l, q, i], hr.at[l, q, i], to_up).wait_recv()
            send_far(l, q, i).start()

    def load_sides(l, q):
        if l > 0:
            for i in range(4):
                output_copy(l - 1, q, i).wait_send()
        for i in (0, 1):
            hidden_load(l, q, i).start()
        for i in (0, 1):
            hidden_load(l, q, i).wait()

    def take_far(l, q):
        for i in (0, 1):
            ref = half(h_land.at[l, q, 2], i)
            remote(ref, ref, hs.at[l, q, 2 + i], hr.at[l, q, 2 + i], to_up).wait_recv()
        hidden_load(l, q, 2).start()
        hidden_load(l, q, 2).wait()

    def clear_acc(q):
        def step(i, carry):
            rows = pl.ds(pl.multiple_of(lax.rem(i, 4) * CHUNK, CHUNK), CHUNK)
            acc[2 * q + i // 4, rows, :] = jnp.zeros((CHUNK, d_model), jnp.float32)
            return carry
        lax.fori_loop(0, 2 * (tok_dev // CHUNK), step, 0)

    def output_copy(l, q, i):
        dev = (to_up, to_down, to_down, to_up, to_up, to_down)[i]
        far = o_land.at[l, q, 2]
        src = (half(place(3, q), 0), half(place(3, q), 1), place(1, q), place(2, q),
               r_land.at[l, q, 0], r_land.at[l, q, 1])[i]
        dst = (r_land.at[l, q, 0], r_land.at[l, q, 1], o_land.at[l, q, 0], o_land.at[l, q, 1],
               half(far, 0), half(far, 1))[i]
        return remote(src, dst, os_.at[l, q, i], or_.at[l, q, i], dev)

    def round_block(block, q):
        for i in range(part // CHUNK):
            rows = pl.ds(block % 2 * part + i * CHUNK, CHUNK)
            h_all[2 * q + block // 2, rows, :] = acc[2 * q + block // 2, rows, :].astype(jnp.bfloat16)

    def issue_outputs(l, q):
        round_block(3, q)
        output_copy(l, q, 0).start()
        output_copy(l, q, 1).start()
        round_block(1, q)
        output_copy(l, q, 2).start()
        round_block(2, q)
        output_copy(l, q, 3).start()

    def relay(l, q):
        for i in (0, 1):
            ref = r_land.at[l, q, i]
            remote(ref, ref, os_.at[l, q, i], or_.at[l, q, i], to_up).wait_recv()
            output_copy(l, q, 4 + i).start()

    def collect(l, q):
        def fetch(i):
            return pltpu.make_async_copy(o_land.at[l, q, i], orecv.at[i], ld.at[4 + i])
        for i in (0, 1):
            ref = o_land.at[l, q, i]
            remote(ref, ref, os_.at[l, q, i], or_.at[l, q, 2 + i], to_up).wait_recv()
            fetch(i).start()
        for i in (0, 1):
            ref = half(o_land.at[l, q, 2], i)
            remote(ref, ref, os_.at[l, q, i], or_.at[l, q, 4 + i], to_up).wait_recv()
        fetch(2).start()
        for i in range(3):
            fetch(i).wait()

    def combine(l, q):
        collect(l, q)
        sources = (up, down, lax.rem(y + 2, n_ep))

        def step(i, carry):
            local = pl.ds(pl.multiple_of(i * CHUNK, CHUNK), CHUNK)
            rows = pl.ds(pl.multiple_of(q * part + i * CHUNK, CHUNK), CHUNK)
            ids, gate = routes_ref[l, rows, :], gates[rows, :]
            id0, id1, gate0, gate1 = ids[:, 0:1], ids[:, 1:2], gate[:, 0:1], gate[:, 1:2]

            def term(expert, value):
                is0, is1 = id0 == expert, id1 == expert
                weight = jnp.where(is0, gate0, gate1)
                return jnp.where(jnp.logical_or(is0, is1), weight * value.astype(jnp.float32), 0.0)
            mixed = term(y, acc[2 * q, local, :].astype(jnp.bfloat16))
            for j, expert in enumerate(sources):
                mixed += term(expert, orecv[j, local, :])
            xs[rows, :] = (xs[rows, :].astype(jnp.float32) + mixed).astype(jnp.bfloat16)
            return carry
        lax.fori_loop(0, part // CHUNK, step, 0)

    def experts(l):
        again = 0 if l == 0 else 12
        steps = 8 if l == 0 else 16

        def slice_at(i):
            return i if l == 0 else jnp.where(i < again, lax.rem(i, 4), i - 8)

        def low(i):
            return jnp.int32(0) if l == 0 else jnp.where(i < again, i // 4, 0)

        def high(i):
            return jnp.int32(4) if l == 0 else jnp.where(i < 4, 1, jnp.where(i < 8, 2, 4))

        def first_use(i):
            return i >= 0 if l == 0 else jnp.logical_or(i < 4, i >= again)

        def prefetch(i):
            waits = (3, 5) if l == 0 else (13,)
            fine = i < steps - 1
            for k in waits:
                fine = jnp.logical_and(fine, i != k)
            return fine

        def ready(i, pieces):
            for s in range(1, 8):
                @pl.when(jnp.logical_and(first_use(i), slice_at(i) == s))
                def _(s=s):
                    for t in pieces:
                        if s % 2:
                            arrived(l, t, s)
                        elif (l, t, s // 2) not in early:
                            pass_ring(l, t, s // 2)

        early = {(0, 0, 1), (0, 1, 1), (0, 2, 1), (1, 0, 1), (1, 1, 1), (1, 2, 1), (1, 0, 2), (1, 1, 2), (1, 2, 2)}

        def at(i, k, action):
            @pl.when(i == k)
            def _():
                action()

        def step(i, carry):
            @pl.when(i < steps)
            def _():
                load13_wait()

            def gate_up(rb, c):
                @pl.when(jnp.logical_and(rb == jnp.where(i == steps - 1, high(i) - 1, low(i)), i > 0))
                def _():
                    ready(i - 1, (2,))
                    load2(l, slice_at(i - 1))

                @pl.when(jnp.logical_and(rb == high(i) - 1, prefetch(i)))
                def _():
                    ready(i + 1, (0, 1))
                    load13(l, slice_at(i + 1), i + 1)
                if l == 0:
                    @pl.when(jnp.logical_and(rb == 3, i == 0))
                    def _():
                        pass_ring(0, 2, 1)
                for c, width in groups[:-1]:
                    last = c + width == main
                    span = pl.ds(2 * c, 2 * width + (2 * tail if last else 0))
                    both = lax.dot_general(h_all[rb], b13[lax.rem(i, 2), span, :], NT,
                                           preferred_element_type=jnp.float32)
                    u, v = both[:, :width], both[:, width:2 * width]
                    act[lax.rem(i, 2), rb, :, c:c + width] = (u * jax.nn.sigmoid(u) * v).astype(jnp.bfloat16)
                    if last:
                        edge = both[:, 2 * width:]
                        rest = edge * jax.nn.sigmoid(edge) * pltpu.roll(edge, tail, 1)
                        act[lax.rem(i, 2), rb, :, main:] = rest[:, :tail].astype(jnp.bfloat16)
                return c
            lax.fori_loop(low(i), jnp.where(i < steps, high(i), low(i)), gate_up, 0)

            @pl.when(i == steps)
            def _():
                ready(i - 1, (2,))
                load2(l, slice_at(i - 1))

            if l == 0:
                @pl.when(i == 5)
                def _():
                    for t in range(3):
                        push_own(1, t)

            def fetch_next(late):
                @pl.when(jnp.logical_and(jnp.logical_and(i < steps - 1, jnp.logical_not(prefetch(i))), (i == 5) == late))
                def _():
                    ready(i + 1, (0, 1))
                    load13(l, slice_at(i + 1), i + 1)

            fetch_next(False)

            @pl.when(i > 0)
            def _():
                load2_wait()

            def down_proj(rb, c):
                cols = 512
                for n in range(d_model // cols):
                    span = pl.ds(n * cols, cols)
                    acc[rb, :, span] += jnp.dot(act[lax.rem(i + 1, 2), rb], b2[:, span],
                                                preferred_element_type=jnp.float32)

                @pl.when(jnp.logical_and(i == steps, rb == 1))
                def _():
                    issue_outputs(l, 0)
                return c
            lax.fori_loop(low(i - 1), jnp.where(i > 0, high(i - 1), low(i - 1)), down_proj, 0)

            fetch_next(True)
            return carry

        def second_half():
            combine(0, 1)
            for i in (0, 1):
                send_side(0, 1, i).wait_send()
            normalise(1, 1)
            send_hidden(1, 1)
            clear_acc(1)
            pass_ring(1, 0, 2)

        def far_rows():
            load_sides(1, 1)
            take_far(1, 1)

        def step_all(i, carry):
            if l == 1:
                at(i, 2, second_half)
                at(i, 4, lambda: take_far(1, 0))
                at(i, 5, lambda: pass_ring(1, 1, 2))
                at(i, 6, lambda: take_sides(1, 1))
                at(i, 8, far_rows)
                at(i, 9, lambda: pass_ring(1, 2, 2))
            return step(i, carry)

        load13(l, 0, jnp.int32(0))
        lax.fori_loop(0, steps + 1, step_all, 0)

    barrier = pltpu.get_barrier_semaphore()
    for dev in (to_next, to_prev, to_partner, to_up, to_down):
        pl.semaphore_signal(barrier, inc=1, device_id=dev, device_id_type=MESH)
    pl.semaphore_wait(barrier, 5)

    for t in range(3):
        push_own(0, t)
    x_copy = pltpu.make_async_copy(x_hbm, xs, ld.at[3])
    x_copy.start()
    x_copy.wait()
    for q in (0, 1):
        normalise(0, q)
        send_hidden(0, q)
    for q in (0, 1):
        take_sides(0, q)
        clear_acc(q)
    pass_ring(0, 0, 1)
    for q in (0, 1):
        load_sides(0, q)
        take_far(0, q)
    pass_ring(0, 1, 1)
    experts(0)

    relay(0, 0)
    issue_outputs(0, 1)
    combine(0, 0)
    for i in (0, 1):
        send_side(0, 0, i).wait_send()
    normalise(1, 0)
    send_hidden(1, 0)
    clear_acc(0)
    relay(0, 1)
    for t in range(3):
        pass_ring(1, t, 1)
    take_sides(1, 0)
    load_sides(1, 0)
    experts(1)

    relay(1, 0)
    issue_outputs(1, 1)
    combine(1, 0)
    outs = [pltpu.make_async_copy(xs.at[pl.ds(q * part, part)], out_hbm.at[pl.ds(q * part, part)], ld.at[2 + q])
            for q in (0, 1)]
    outs[0].start()
    relay(1, 1)
    combine(1, 1)
    outs[1].start()
    for l in range(layers):
        for t in range(3):
            for r in range(3):
                ring_send(l, t, r).wait_send()
            for r in range(4):
                partner_send(l, t, r).wait_send()
        for q in (0, 1):
            for i in (0, 1):
                if l == 1:
                    send_side(l, q, i).wait_send()
                send_far(l, q, i).wait_send()
            for i in range(4 if l == 1 else 0):
                output_copy(l, q, i).wait_send()
            for i in (4, 5):
                output_copy(l, q, i).wait_send()
    outs[0].wait()
    outs[1].wait()


def solution(mesh):
    n_ep, n_fs = mesh.shape["ep"], mesh.shape["fsdp"]
    token_spec = P(("rep", "ep", "fsdp"), None)
    expert_in_spec = P(None, "ep", None, "fsdp")
    expert_out_spec = P(None, "ep", "fsdp", None)
    route_spec = P(None, ("rep", "ep", "fsdp"), None)

    def device_step(x_in, norm_w, router_w, gate_w, up_w, down_w, routes):
        layers, tok_dev, top_k = routes.shape
        d_model = x_in.shape[1]
        ff = down_w.shape[2]
        bf16 = jnp.bfloat16
        hbm, vmem = pl.BlockSpec(memory_space=pl.ANY), pl.BlockSpec(memory_space=pltpu.VMEM)
        shape = jax.ShapeDtypeStruct
        outs = pl.pallas_call(
            functools.partial(kernel, n_ep, n_fs),
            name="moe_layers",
            out_shape=(shape((tok_dev, d_model), bf16),
                       shape((layers, n_fs, ff, d_model), bf16),
                       shape((layers, n_fs, ff, d_model), bf16),
                       shape((layers, n_fs, ff, d_model), bf16),
                       shape((layers, 2, 3, tok_dev // 2, d_model), bf16),
                       shape((layers, 2, 3, tok_dev // 2, d_model), bf16),
                       shape((layers, 2, 2, tok_dev // 4, d_model), bf16)),
            in_specs=[hbm, vmem, vmem, hbm, hbm, hbm, vmem],
            out_specs=(hbm,) * 7,
            scratch_shapes=[
                pltpu.VMEM((4, tok_dev, d_model), bf16),
                pltpu.VMEM((4, tok_dev, d_model), jnp.float32),
                pltpu.VMEM((2, 2 * ff, d_model), bf16),
                pltpu.VMEM((ff, d_model), bf16),
                pltpu.VMEM((2, 4, tok_dev, ff), bf16),
                pltpu.VMEM((tok_dev, d_model), bf16),
                pltpu.VMEM((3, tok_dev // 2, d_model), bf16),
                pltpu.VMEM((tok_dev, 128), jnp.float32),
                pltpu.SemaphoreType.DMA((layers, 3, 7)),
                pltpu.SemaphoreType.DMA((layers, 3, 8)),
                pltpu.SemaphoreType.DMA((layers, 2, 4)),
                pltpu.SemaphoreType.DMA((layers, 2, 4)),
                pltpu.SemaphoreType.DMA((layers, 2, 6)),
                pltpu.SemaphoreType.DMA((layers, 2, 6)),
                pltpu.SemaphoreType.DMA((10,)),
            ],
            compiler_params=pltpu.CompilerParams(collective_id=0, has_side_effects=True,
                                                 vmem_limit_bytes=66_000_000),
        )(x_in, norm_w, jnp.swapaxes(router_w, 1, 2), jnp.swapaxes(gate_w, 2, 3), jnp.swapaxes(up_w, 2, 3), down_w, routes)
        return outs[0]

    return jax.shard_map(device_step, mesh=mesh,
                         in_specs=(token_spec, P(), P(), expert_in_spec, expert_in_spec, expert_out_spec, route_spec),
                         out_specs=token_spec, check_vma=False)
```
